8 devices in a mesh: col: 2 (over z, y), row: 4 (over x, core).
Axes of the slice: x: 2, y: 2, z: 1, core: 2. Of those that a mesh axis runs over, the one named last changes fastest.
Arguments:
- adjacency: bfloat16 [16384, 16384], P('row', 'col')
- pers_vec: float32 [16384, 128], P(('row', 'col'))
- restart_wt: float32 [32, 128], replicated
Outputs:
- output 1: float32 [16384, 128], P(('col', 'row'))
- output 2: float32 [16384, 128], P(('row', 'col'))
All inputs are finite; a program needn't handle non-finite values.
Results may differ from the reference program's by a relative error of at most 0.001.
Values are sent between devices in bfloat16 or wider.
A program may use at most 1 GiB of HBM per device.

```python
import jax
import jax.numpy as jnp
from jax import lax

N = 16384
DEG = 16
M = 128
SWEEPS = 32


def setup_inputs(seed: int = 0) -> dict:
    base_key = jax.random.key(seed)
    k_out, k_pop, k_adj, k_start, k_val, k_rest = jax.random.split(base_key, 6)
    out_budget = jax.random.randint(k_out, (N,), 1, 2 * DEG + 1)
    popularity = jax.random.randint(k_pop, (N,), 1, 16)
    row_count = N // 16

    def draw_rows(block_idx):
        draw_bits = jax.random.randint(jax.random.fold_in(k_adj, block_idx), (row_count, N), 0, 8 * N)
        pop_rows = lax.dynamic_slice(popularity, (block_idx * row_count,), (row_count,))
        return (draw_bits < pop_rows[:, None] * out_budget[None, :]).astype(jnp.bfloat16)

    adjacency = lax.map(draw_rows, jnp.arange(16)).reshape(N, N)
    win_start = jax.random.randint(k_start, (M,), 0, N)
    inside = ((jnp.arange(N)[:, None] - win_start[None, :]) % N) < (N // 8)
    raw_vals = jnp.abs(jax.random.normal(k_val, (N, M), jnp.float32)) * jnp.where(inside, 1.0, 0.05)
    pers_vec = raw_vals * lax.rsqrt(jnp.mean(raw_vals * raw_vals, axis=0, keepdims=True))
    restart_wt = jax.random.uniform(k_rest, (SWEEPS, M), jnp.float32, 0.15, 0.45)
    return {"adjacency": adjacency, "pers_vec": pers_vec, "restart_wt": restart_wt}


def col_normalise(vals):
    return vals * lax.rsqrt(jnp.mean(vals * vals, axis=0, keepdims=True))


def reference(adjacency, pers_vec, restart_wt):
    def sweep(carry, weight):
        hub_vec = carry[0]
        auth_prod = lax.dot_general(adjacency, hub_vec.astype(jnp.bfloat16), (((0,), (0,)), ((), ())), preferred_element_type=jnp.float32)
        auth_vec = col_normalise(auth_prod)
        hub_prod = jnp.dot(adjacency, auth_vec.astype(jnp.bfloat16), preferred_element_type=jnp.float32)
        hub_new = (1.0 - weight) * col_normalise(hub_prod) + weight * pers_vec
        return (hub_new, auth_vec), None

    final_state, unused_out = lax.scan(sweep, (pers_vec, jnp.zeros_like(pers_vec)), restart_wt)
    return final_state[1], final_state[0]
```

```python
import jax
import jax.numpy as jnp
from jax import lax
from jax.experimental import pallas as pl
from jax.experimental.pallas import tpu as pltpu
from jax.sharding import PartitionSpec as P

MESH = pl.DeviceIdType.MESH
F32 = jnp.float32
BF16 = jnp.bfloat16
GROUPS = 2
RING = 3


def dot_plain(lhs, rhs):
    return lax.dot_general(lhs, rhs, (((1,), (0,)), ((), ())), preferred_element_type=F32)


def dot_trans(lhs, rhs):
    return lax.dot_general(lhs, rhs, (((1,), (1,)), ((), ())), preferred_element_type=F32)


def make_kernel(sweeps, n_total, piece, half_len, m):
    n_blocks = sweeps * 32
    step_len = 512
    n_steps = piece // step_len
    steps_half = half_len // step_len

    def kernel(adj, adj_t, start, weights, auth_out, hub_out, res, ring, part, pair_recv, recv, auth, hub, norm_send, norm_recv,
               res_sem, ring_sem, pair_ss, pair_rs, link_ss, link_rs, norm_ss, norm_rs, auth_ss, auth_rs, hub_ss, hub_rs):
        j = lax.axis_index("col")
        i = lax.axis_index("row")
        x = i // 2
        c = i % 2
        own_row = pl.multiple_of(j * piece, piece)
        far_row = pl.multiple_of((1 - j) * piece, piece)
        pair_dev = (j, 2 * x + 1 - c)
        x_dev = (j, 2 * (1 - x) + c)
        y_dev = (1 - j, i)

        def piece_of(px, pc):
            return pl.ds(pl.multiple_of((2 * px + pc) * piece, piece), piece)

        own_cols = piece_of(x, c)
        pair_cols = piece_of(x, 1 - c)
        far_cols = piece_of(1 - x, c)
        far_pair_cols = piece_of(1 - x, 1 - c)

        def relative(r):
            rj, rx, rc = r // 4, (r // 2) % 2, r % 2
            jj = 1 - j if rj else j
            xx = 1 - x if rx else x
            cc = 1 - c if rc else c
            return (jj, 2 * xx + cc)

        def remote(src, dst, ss, rs, dev):
            return pltpu.make_async_remote_copy(src_ref=src, dst_ref=dst, send_sem=ss, recv_sem=rs, device_id=dev, device_id_type=MESH)

        def pair_copy(g, slot, half):
            return remote(part.at[g, 2 * slot, half], pair_recv.at[g, slot, half], pair_ss.at[g, slot, half], pair_rs.at[g, slot, half], pair_dev)

        def x_copy(g, half):
            return remote(part.at[g, 1, half], recv.at[g, half], link_ss.at[0, g, half], link_rs.at[0, g, half], x_dev)

        def y_copy(g, half):
            return remote(part.at[g, 0, half], recv.at[g, half], link_ss.at[1, g, half], link_rs.at[1, g, half], y_dev)

        def norm_copy(phase, g, r):
            return remote(norm_send.at[phase, g], norm_recv.at[phase, g, r - 1], norm_ss.at[phase, g, r - 1], norm_rs.at[phase, g, r - 1], relative(r))

        def auth_pair(g):
            return remote(auth.at[g, :, own_cols], auth.at[g, :, own_cols], auth_ss.at[g, 0], auth_rs.at[g, 0], pair_dev)

        def auth_x(g):
            return remote(auth.at[g, :, own_cols], auth.at[g, :, own_cols], auth_ss.at[g, 1], auth_rs.at[g, 1], x_dev)

        def auth_forward(g):
            return remote(auth.at[g, :, far_cols], auth.at[g, :, far_cols], auth_ss.at[g, 2], auth_rs.at[g, 2], pair_dev)

        def hub_y(g):
            return remote(hub.at[g, 0], hub.at[g, 1], hub_ss.at[g], hub_rs.at[g], y_dev)

        def block_copy(t, first):
            buf = t % RING
            b = t % 8
            if first:
                o = b // 2
                cols = (2 * ((x + 1 - o // 2) % 2) + (c + 1 + o) % 2) * piece + (b % 2) * half_len
                src = adj.at[pl.ds(far_row, piece), pl.ds(pl.multiple_of(cols, half_len), half_len)]
            else:
                kp = b % 4
                rows = (2 * ((x + kp // 2) % 2) + (c + kp) % 2) * piece
                cols = (b // 4) * half_len
                src = adj_t.at[pl.ds(pl.multiple_of(rows, piece), piece), pl.ds(pl.multiple_of(cols, half_len), half_len)]
            return pltpu.make_async_copy(src, ring.at[buf], ring_sem.at[buf])

        def block_start(t):
            first = (t // 8) % 4 < 2

            @pl.when(jnp.logical_and(t < n_blocks, first))
            def _():
                block_copy(t, True).start()

            @pl.when(jnp.logical_and(t < n_blocks, jnp.logical_not(first)))
            def _():
                block_copy(t, False).start()

        def sum_squares(vals):
            sq = None
            for val in vals:
                val = val * val
                for q in range(half_len // 128):
                    cur = val[:, q * 128:(q + 1) * 128]
                    sq = cur if sq is None else sq + cur
            padded = jnp.concatenate([sq, jnp.zeros((128 - m, 128), F32)], axis=0)
            return jnp.sum(padded.T, axis=0, keepdims=True)

        def spread(row):
            return jnp.broadcast_to(row, (128, 128)).T

        def norm_start(phase, g, vals):
            norm_send[phase, g] = jnp.broadcast_to(sum_squares(vals), (8, 128))
            for r in range(1, 8):
                norm_copy(phase, g, r).start()

        def norm_finish(phase, g):
            total = norm_send[phase, g]
            for r in range(1, 8):
                norm_copy(phase, g, r).wait_recv()
                total = total + norm_recv[phase, g, r - 1]
            for r in range(1, 8):
                norm_copy(phase, g, r).wait_send()
            return spread(lax.rsqrt(total[0:1, :] / n_total))[:m, 0:1]

        def auth_sum(g):
            vals = []
            for half in range(2):
                pair_copy(g, 1, half).wait_recv()
                x_copy(g, half).wait_recv()
                val = part[g, 3, half] + pair_recv[g, 1, half] + recv[g, half]
                part[g, 3, half] = val
                vals.append(val)
            norm_start(0, g, vals)

        def auth_finish(g):
            scale = norm_finish(0, g)
            for half in range(2):
                val = part[g, 3, half] * scale
                cols = pl.ds(half * half_len, half_len)
                auth_out[g, :, cols] = val
                base = pl.multiple_of((2 * x + c) * piece + half * half_len, half_len)
                auth[g, :, pl.ds(base, half_len)] = val.astype(BF16)
            auth_x(g).start()
            auth_pair(g).start()
            for half in range(2):
                pair_copy(g, 0, half).wait_send()
                pair_copy(g, 1, half).wait_send()
                x_copy(g, half).wait_send()

        def hub_sum(g):
            vals = []
            for half in range(2):
                y_copy(g, half).wait_recv()
                val = part[g, 3, half] + recv[g, half]
                part[g, 3, half] = val
                vals.append(val)
            norm_start(1, g, vals)

        def hub_finish(g, k, send):
            scale = norm_finish(1, g)
            row = weights[g, pl.ds(k, 1), :]
            weight = spread(row)[:m, 0:1]
            for half in range(2):
                cols = pl.ds(half * half_len, half_len)
                val = (1.0 - weight) * (part[g, 3, half] * scale) + weight * start[g, :, cols]
                hub_out[g, :, cols] = val
                hub[g, 0, :, cols] = val.astype(BF16)

            if send is not None:
                @pl.when(send)
                def _():
                    hub_y(g).start()

            for half in range(2):
                y_copy(g, half).wait_send()
            auth_pair(g).wait_send()
            auth_x(g).wait_send()
            auth_forward(g).wait_send()

        barrier = pltpu.get_barrier_semaphore()
        for r in range(1, 8):
            pl.semaphore_signal(barrier, inc=1, device_id=relative(r), device_id_type=MESH)
        pl.semaphore_wait(barrier, 7)

        res_copy = pltpu.make_async_copy(adj.at[pl.ds(own_row, piece), :], res, res_sem)
        res_copy.start()
        for t in range(RING):
            block_copy(t, True).start()
        for g in range(GROUPS):
            hub[g, 0] = start[g].astype(BF16)
            hub_y(g).start()
        res_copy.wait()

        def sweep(k, carry):
            base = k * 32

            def first_product(g, carry):
                def chunk(b, carry):
                    t = base + g * 8 + b
                    o, half = b // 2, b % 2
                    cols = (2 * ((x + 1 - o // 2) % 2) + (c + 1 + o) % 2) * piece + half * half_len

                    @pl.when(b == 0)
                    def _():
                        hub_y(g).wait()

                    block_copy(t, True).wait()
                    acc = dot_plain(hub[g, 1], ring[t % RING])
                    acc = acc + dot_plain(hub[g, 0], res[:, pl.ds(pl.multiple_of(cols, half_len), half_len)])
                    part[g, o, half] = acc
                    block_start(t + RING)

                    @pl.when(o == 0)
                    def _():
                        pair_copy(g, 0, half).start()

                    @pl.when(jnp.logical_and(b == 1, jnp.logical_and(g == 0, k > 0)))
                    def _():
                        hub_sum(1)

                    @pl.when(jnp.logical_and(b == 3, jnp.logical_and(g == 0, k > 0)))
                    def _():
                        hub_finish(1, k - 1, k > 0)

                    @pl.when(jnp.logical_and(b == 1, g == 1))
                    def _():
                        auth_sum(0)

                    @pl.when(jnp.logical_and(b == 3, g == 1))
                    def _():
                        auth_finish(0)

                    @pl.when(o == 1)
                    def _():
                        pair_copy(g, 0, half).wait_recv()
                        part[g, 1, half] = part[g, 1, half] + pair_recv[g, 0, half]
                        x_copy(g, half).start()

                    @pl.when(o == 2)
                    def _():
                        pair_copy(g, 1, half).start()

                    return carry

                return lax.fori_loop(0, 8, chunk, carry)

            lax.fori_loop(0, GROUPS, first_product, 0)

            def second_product(g, carry):
                def row_half(half, carry):
                    for kp in range(4):
                        t = base + 16 + g * 8 + half * 4 + kp
                        if kp == 1:
                            @pl.when(half == 0)
                            def _():
                                auth_pair(g).wait_recv()
                                auth_x(g).wait_recv()
                                auth_forward(g).start()
                        if kp == 3:
                            @pl.when(half == 0)
                            def _():
                                auth_forward(g).wait_recv()
                        block_copy(t, False).wait()
                        lhs = auth[g, :, (own_cols, pair_cols, far_cols, far_pair_cols)[kp]]
                        acc = dot_plain(lhs, ring[t % RING])
                        if kp:
                            acc = acc + part[g, 0, half]
                        part[g, 0, half] = acc
                        block_start(t + RING)
                    y_copy(g, half).start()

                    @pl.when(jnp.logical_and(half == 0, g == 1))
                    def _():
                        hub_sum(0)

                    @pl.when(jnp.logical_and(half == 1, g == 1))
                    def _():
                        hub_finish(0, k, k < sweeps - 1)

                    @pl.when(jnp.logical_and(half == 1, g == 0))
                    def _():
                        auth_sum(1)

                    return carry

                lax.fori_loop(0, 2, row_half, 0)

                def own_step(q, carry):
                    rows = pl.ds(pl.multiple_of(q * step_len, step_len), step_len)
                    cols = pl.ds(pl.multiple_of((q % steps_half) * step_len, step_len), step_len)
                    part[g, 3, q // steps_half, :, cols] = dot_trans(auth[g], res[rows, :])

                    @pl.when(jnp.logical_and(q == 1, g == 0))
                    def _():
                        auth_finish(1)

                    return carry

                return lax.fori_loop(0, n_steps, own_step, carry)

            lax.fori_loop(0, GROUPS, second_product, 0)
            return carry

        lax.fori_loop(0, sweeps, sweep, 0)
        hub_sum(1)
        hub_finish(1, sweeps - 1, None)

    return kernel


def solution(mesh):
    col_size = mesh.shape["col"]
    row_size = mesh.shape["row"]

    def device_fn(adj_tile, pers_piece, restart_wt):
        rows, n_cols = adj_tile.shape
        n_total = rows * row_size
        piece, width = pers_piece.shape
        sweeps = restart_wt.shape[0]
        m = width // GROUPS
        half_len = piece // 2
        far = 1 - lax.axis_index("col")
        adj_t = lax.dynamic_slice(adj_tile, (far * piece, 0), (piece, n_cols)).T
        start = pers_piece.T.reshape(GROUPS, m, piece)
        weights = restart_wt.reshape(sweeps, GROUPS, m).transpose(1, 0, 2)
        weights = jnp.pad(weights, ((0, 0), (0, 0), (0, 128 - m)))
        vmem = pl.BlockSpec(memory_space=pltpu.VMEM)
        hbm = pl.BlockSpec(memory_space=pl.ANY)
        dma = pltpu.SemaphoreType.DMA
        auth_t, hub_t = pl.pallas_call(
            make_kernel(sweeps, n_total, piece, half_len, m),
            out_shape=[jax.ShapeDtypeStruct((GROUPS, m, piece), F32)] * 2,
            in_specs=[hbm, hbm, vmem, vmem],
            out_specs=[vmem, vmem],
            scratch_shapes=[
                pltpu.VMEM((piece, n_cols), BF16),
                pltpu.VMEM((RING, piece, half_len), BF16),
                pltpu.VMEM((GROUPS, 4, 2, m, half_len), F32),
                pltpu.VMEM((GROUPS, 2, 2, m, half_len), F32),
                pltpu.VMEM((GROUPS, 2, m, half_len), F32),
                pltpu.VMEM((GROUPS, m, n_cols), BF16),
                pltpu.VMEM((GROUPS, 2, m, piece), BF16),
                pltpu.VMEM((2, GROUPS, 8, 128), F32),
                pltpu.VMEM((2, GROUPS, 7, 8, 128), F32),
                dma,
                dma((RING,)),
                dma((GROUPS, 2, 2)),
                dma((GROUPS, 2, 2)),
                dma((2, GROUPS, 2)),
                dma((2, GROUPS, 2)),
                dma((2, GROUPS, 7)),
                dma((2, GROUPS, 7)),
                dma((GROUPS, 3)),
                dma((GROUPS, 3)),
                dma((GROUPS,)),
                dma((GROUPS,)),
            ],
            compiler_params=pltpu.CompilerParams(collective_id=0, has_side_effects=True, vmem_limit_bytes=67000000),
            name="hits_sweeps",
        )(adj_tile, adj_t, start, weights)
        return auth_t.reshape(width, piece).T, hub_t.reshape(width, piece).T

    return jax.shard_map(device_fn, mesh=mesh, in_specs=(P("row", "col"), P(("row", "col"), None), P(None, None)), out_specs=(P(("col", "row"), None), P(("row", "col"), None)), check_vma=False)
```

```python
import jax
import jax.numpy as jnp
from jax import lax
from jax.experimental import pallas as pl
from jax.experimental.pallas import tpu as pltpu
from jax.sharding import PartitionSpec as P

MESH = pl.DeviceIdType.MESH
F32 = jnp.float32
BF16 = jnp.bfloat16
GROUPS = 2
RING = 4
HOOKS = (-1, 1, 5, 8, -1, 5, 1, 3)


def dot_plain(lhs, rhs):
    lhs = jnp.concatenate([lhs, lhs], axis=0)
    out = lax.dot_general(lhs, rhs, (((1,), (0,)), ((), ())), preferred_element_type=F32)
    return out[:lhs.shape[0] // 2]


def dot_trans(lhs, rhs):
    return lax.dot_general(lhs, rhs, (((1,), (1,)), ((), ())), preferred_element_type=F32)


def make_kernel(sweeps, n_total, piece, half_len, m):
    n_slots = sweeps * 4
    n_blocks = n_slots * 8
    step_len = 512
    steps_half = half_len // step_len
    n_steps = piece // step_len

    def kernel(adj, adj_t, start, weights, auth_out, hub_out, res, ring, part, pair_recv, recv, auth, hub, norm_send, norm_recv,
               res_sem, ring_sem, pair_ss, pair_rs, link_ss, link_rs, norm_ss, norm_rs, auth_ss, auth_rs, hub_ss, hub_rs):
        j = lax.axis_index("col")
        i = lax.axis_index("row")
        x = i // 2
        c = i % 2
        own_row = pl.multiple_of(j * piece, piece)
        far_row = pl.multiple_of((1 - j) * piece, piece)
        pair_dev = (j, 2 * x + 1 - c)
        x_dev = (j, 2 * (1 - x) + c)
        y_dev = (1 - j, i)

        def piece_of(px, pc):
            return pl.ds(pl.multiple_of((2 * px + pc) * piece, piece), piece)

        own_cols = piece_of(x, c)
        pair_cols = piece_of(x, 1 - c)
        far_cols = piece_of(1 - x, c)
        far_pair_cols = piece_of(1 - x, 1 - c)

        def relative(r):
            rj, rx, rc = r // 4, (r // 2) % 2, r % 2
            jj = 1 - j if rj else j
            xx = 1 - x if rx else x
            cc = 1 - c if rc else c
            return (jj, 2 * xx + cc)

        def remote(src, dst, ss, rs, dev):
            return pltpu.make_async_remote_copy(src_ref=src, dst_ref=dst, send_sem=ss, recv_sem=rs, device_id=dev, device_id_type=MESH)

        def pair_copy(g, slot, half):
            return remote(part.at[g, 2 * slot, half], pair_recv.at[g, slot, half], pair_ss.at[g, slot, half], pair_rs.at[g, slot, half], pair_dev)

        def x_copy(g, half):
            return remote(part.at[g, 1, half], recv.at[g, half], link_ss.at[0, g, half], link_rs.at[0, g, half], x_dev)

        def y_copy(g, half):
            return remote(part.at[g, 0, half], recv.at[g, half], link_ss.at[1, g, half], link_rs.at[1, g, half], y_dev)

        def norm_copy(phase, g, r):
            return remote(norm_send.at[phase, g], norm_recv.at[phase, g, r - 1], norm_ss.at[phase, g, r - 1], norm_rs.at[phase, g, r - 1], relative(r))

        def auth_pair(g):
            return remote(auth.at[g, :, own_cols], auth.at[g, :, own_cols], auth_ss.at[g, 0], auth_rs.at[g, 0], pair_dev)

        def auth_x(g):
            return remote(auth.at[g, :, own_cols], auth.at[g, :, own_cols], auth_ss.at[g, 1], auth_rs.at[g, 1], x_dev)

        def auth_forward(g):
            return remote(auth.at[g, :, far_cols], auth.at[g, :, far_cols], auth_ss.at[g, 2], auth_rs.at[g, 2], pair_dev)

        def hub_y(g):
            return remote(hub.at[g, 0], hub.at[g, 1], hub_ss.at[g], hub_rs.at[g], y_dev)

        def chunk_of(b):
            late = b // 4
            o = (1 - late) * (b % 2) + late * (b // 2)
            half = (1 - late) * (b // 2) + late * (b % 2)
            cols = (2 * ((x + 1 - o // 2) % 2) + (c + 1 + o) % 2) * piece + half * half_len
            return o, half, cols

        def block_copy(t, first):
            buf = t % RING
            b = t % 8
            if first:
                _, _, cols = chunk_of(b)
                src = adj.at[pl.ds(far_row, piece), pl.ds(pl.multiple_of(cols, half_len), half_len)]
            else:
                kp = b % 4
                rows = (2 * ((x + kp // 2) % 2) + (c + kp) % 2) * piece
                cols = (b // 4) * half_len
                src = adj_t.at[pl.ds(pl.multiple_of(rows, piece), piece), pl.ds(pl.multiple_of(cols, half_len), half_len)]
            return pltpu.make_async_copy(src, ring.at[buf], ring_sem.at[buf])

        def block_start(t):
            u = t // 8
            place = (u + 1) % 4
            first = jnp.logical_and(jnp.logical_or(jnp.logical_or(place == 0, place == 3), u == 0), u < n_slots - 1)

            @pl.when(jnp.logical_and(t < n_blocks, first))
            def _():
                block_copy(t, True).start()

            @pl.when(jnp.logical_and(t < n_blocks, jnp.logical_not(first)))
            def _():
                block_copy(t, False).start()

        def sum_squares(vals):
            sq = None
            for val in vals:
                val = val * val
                for q in range(half_len // 128):
                    cur = val[:, q * 128:(q + 1) * 128]
                    sq = cur if sq is None else sq + cur
            padded = jnp.concatenate([sq, jnp.zeros((128 - m, 128), F32)], axis=0)
            return jnp.sum(padded.T, axis=0, keepdims=True)

        def spread(row):
            return jnp.broadcast_to(row, (128, 128)).T

        def norm_start(phase, g, vals):
            norm_send[phase, g] = jnp.broadcast_to(sum_squares(vals), (8, 128))
            for r in range(1, 8):
                norm_copy(phase, g, r).start()

        def norm_finish(phase, g):
            total = norm_send[phase, g]
            for r in range(1, 8):
                norm_copy(phase, g, r).wait_recv()
                total = total + norm_recv[phase, g, r - 1]
            for r in range(1, 8):
                norm_copy(phase, g, r).wait_send()
            return spread(lax.rsqrt(total[0:1, :] / n_total))[:m, 0:1]

        def auth_sum(g):
            vals = []
            for half in range(2):
                pair_copy(g, 1, half).wait_recv()
                x_copy(g, half).wait_recv()
                val = part[g, 3, half] + pair_recv[g, 1, half] + recv[g, half]
                part[g, 3, half] = val
                vals.append(val)
            norm_start(0, g, vals)

        def auth_finish(g):
            scale = norm_finish(0, g)
            for half in range(2):
                val = part[g, 3, half] * scale
                cols = pl.ds(half * half_len, half_len)
                auth_out[g, :, cols] = val
                base = pl.multiple_of((2 * x + c) * piece + half * half_len, half_len)
                auth[g, :, pl.ds(base, half_len)] = val.astype(BF16)
            auth_x(g).start()
            auth_pair(g).start()
            for half in range(2):
                pair_copy(g, 0, half).wait_send()
                pair_copy(g, 1, half).wait_send()
                x_copy(g, half).wait_send()

        def hub_sum(g):
            vals = []
            for half in range(2):
                y_copy(g, half).wait_recv()
                val = part[g, 3, half] + recv[g, half]
                part[g, 3, half] = val
                vals.append(val)
            norm_start(1, g, vals)

        def hub_finish(g, k, send):
            scale = norm_finish(1, g)
            row = weights[g, pl.ds(k, 1), :]
            weight = spread(row)[:m, 0:1]
            for half in range(2):
                cols = pl.ds(half * half_len, half_len)
                val = (1.0 - weight) * (part[g, 3, half] * scale) + weight * start[g, :, cols]
                hub_out[g, :, cols] = val
                hub[g, 0, :, cols] = val.astype(BF16)

            if send is not None:
                @pl.when(send)
                def _():
                    hub_y(g).start()

            for half in range(2):
                y_copy(g, half).wait_send()
            auth_pair(g).wait_send()
            auth_x(g).wait_send()
            auth_forward(g).wait_send()

        barrier = pltpu.get_barrier_semaphore()
        for r in range(1, 8):
            pl.semaphore_signal(barrier, inc=1, device_id=relative(r), device_id_type=MESH)
        pl.semaphore_wait(barrier, 7)

        res_copy = pltpu.make_async_copy(adj.at[pl.ds(own_row, piece), :], res, res_sem)
        res_copy.start()
        for t in range(RING):
            block_copy(t, True).start()
        for g in range(GROUPS):
            hub[g, 0] = start[g].astype(BF16)
            hub_y(g).start()
        res_copy.wait()

        def first_product(g, u, hooks):
            for at, cond, fn in hooks:
                if at < 0:
                    pl.when(cond)(fn)

            def chunk(b, carry):
                t = u * 8 + b
                o, half, cols = chunk_of(b)

                part[g, o, half] = dot_plain(hub[g, 0], res[:, pl.ds(pl.multiple_of(cols, half_len), half_len)])

                @pl.when(b == 0)
                def _():
                    hub_y(g).wait()

                block_copy(t, True).wait()
                part[g, o, half] = part[g, o, half] + dot_plain(hub[g, 1], ring[t % RING])
                block_start(t + RING)

                @pl.when(o == 0)
                def _():
                    pair_copy(g, 0, half).start()

                for at, cond, fn in hooks:
                    if at >= 0:
                        pl.when(jnp.logical_and(b == at, cond))(fn)

                @pl.when(o == 1)
                def _():
                    pair_copy(g, 0, half).wait_recv()
                    part[g, 1, half] = part[g, 1, half] + pair_recv[g, 0, half]
                    x_copy(g, half).start()

                @pl.when(o == 2)
                def _():
                    pair_copy(g, 1, half).start()

                return carry

            lax.fori_loop(0, 8, chunk, 0)

        def second_product(g, u, hooks):
            for at, cond, fn in hooks:
                if at < 0:
                    pl.when(cond)(fn)

            def row_half(half, carry):
                for kp in range(4):
                    t = u * 8 + half * 4 + kp
                    if kp == 1:
                        @pl.when(half == 0)
                        def _():
                            auth_pair(g).wait_recv()
                    if kp == 2:
                        @pl.when(half == 0)
                        def _():
                            auth_x(g).wait_recv()
                            auth_forward(g).start()
                    if kp == 3:
                        @pl.when(half == 0)
                        def _():
                            auth_forward(g).wait_recv()
                    block_copy(t, False).wait()
                    lhs_base = (2 * ((x + kp // 2) % 2) + (c + kp) % 2) * piece

                    acc = dot_plain(auth[g, :, pl.ds(pl.multiple_of(lhs_base, piece), piece)], ring[t % RING])
                    if kp:
                        acc = acc + part[g, 0, half]
                    part[g, 0, half] = acc
                    block_start(t + RING)
                    for at, cond, fn in hooks:
                        if 0 <= at < 8 and at % 4 == kp:
                            pl.when(jnp.logical_and(half == at // 4, cond))(fn)
                y_copy(g, half).start()
                return carry

            lax.fori_loop(0, 2, row_half, 0)

            def own_step(q, carry):
                row = pl.multiple_of(q * step_len, step_len)

                cols = pl.ds(pl.multiple_of((q % steps_half) * step_len, step_len), step_len)
                part[g, 3, q // steps_half, :, cols] = dot_trans(auth[g], res[pl.ds(row, step_len), :])
                for at, cond, fn in hooks:
                    if at >= 8:
                        pl.when(jnp.logical_and(q == at - 8, cond))(fn)
                return carry

            lax.fori_loop(0, n_steps, own_step, 0)

        def sweep(k, carry):
            some, more = k > 0, k < sweeps

            @pl.when(more)
            def _():
                hooks = [(HOOKS[0], some, lambda: auth_sum(1)), (HOOKS[1], some, lambda: auth_finish(1))]
                first_product(0, 4 * k - 1 + 1 // (k + 1), hooks)

            @pl.when(jnp.logical_not(more))
            def _():
                auth_sum(1)
                auth_finish(1)

            @pl.when(jnp.logical_not(some))
            def _():
                auth_sum(0)
                auth_finish(0)

            @pl.when(some)
            def _():
                hooks = [(HOOKS[2], more, lambda: auth_sum(0)), (HOOKS[3], more, lambda: auth_finish(0))]
                second_product(1, 4 * k - k // sweeps, hooks)

            @pl.when(more)
            def _():
                hooks = [(HOOKS[4], some, lambda: hub_sum(1)), (HOOKS[5], some, lambda: hub_finish(1, k - 1, some))]
                second_product(0, 4 * k + 1, hooks)
                hooks = [(HOOKS[6], more, lambda: hub_sum(0)), (HOOKS[7], more, lambda: hub_finish(0, k, k < sweeps - 1))]
                first_product(1, 4 * k + 2, hooks)

            return carry

        lax.fori_loop(0, sweeps + 1, sweep, 0)
        hub_sum(1)
        hub_finish(1, sweeps - 1, None)

    return kernel


def solution(mesh):
    col_size = mesh.shape["col"]
    row_size = mesh.shape["row"]

    def device_fn(adj_tile, pers_piece, restart_wt):
        rows, n_cols = adj_tile.shape
        n_total = rows * row_size
        piece, width = pers_piece.shape
        sweeps = restart_wt.shape[0]
        m = width // GROUPS
        half_len = piece // 2
        far = 1 - lax.axis_index("col")
        adj_t = lax.dynamic_slice(adj_tile, (far * piece, 0), (piece, n_cols)).T
        start = pers_piece.T.reshape(GROUPS, m, piece)
        weights = restart_wt.reshape(sweeps, GROUPS, m).transpose(1, 0, 2)
        weights = jnp.pad(weights, ((0, 0), (0, 0), (0, 128 - m)))
        vmem = pl.BlockSpec(memory_space=pltpu.VMEM)
        hbm = pl.BlockSpec(memory_space=pl.ANY)
        dma = pltpu.SemaphoreType.DMA
        auth_t, hub_t = pl.pallas_call(
            make_kernel(sweeps, n_total, piece, half_len, m),
            out_shape=[jax.ShapeDtypeStruct((GROUPS, m, piece), F32)] * 2,
            in_specs=[hbm, hbm, vmem, vmem],
            out_specs=[vmem, vmem],
            scratch_shapes=[
                pltpu.VMEM((piece, n_cols), BF16),
                pltpu.VMEM((RING, piece, half_len), BF16),
                pltpu.VMEM((GROUPS, 4, 2, m, half_len), F32),
                pltpu.VMEM((GROUPS, 2, 2, m, half_len), F32),
                pltpu.VMEM((GROUPS, 2, m, half_len), F32),
                pltpu.VMEM((GROUPS, m, n_cols), BF16),
                pltpu.VMEM((GROUPS, 2, m, piece), BF16),
                pltpu.VMEM((2, GROUPS, 8, 128), F32),
                pltpu.VMEM((2, GROUPS, 7, 8, 128), F32),
                dma,
                dma((RING,)),
                dma((GROUPS, 2, 2)),
                dma((GROUPS, 2, 2)),
                dma((2, GROUPS, 2)),
                dma((2, GROUPS, 2)),
                dma((2, GROUPS, 7)),
                dma((2, GROUPS, 7)),
                dma((GROUPS, 3)),
                dma((GROUPS, 3)),
                dma((GROUPS,)),
                dma((GROUPS,)),
            ],
            compiler_params=pltpu.CompilerParams(collective_id=0, has_side_effects=True, vmem_limit_bytes=67000000),
            name="hits_sweeps",
        )(adj_tile, adj_t, start, weights)
        return auth_t.reshape(width, piece).T, hub_t.reshape(width, piece).T

    return jax.shard_map(device_fn, mesh=mesh, in_specs=(P("row", "col"), P(("row", "col"), None), P(None, None)), out_specs=(P(("col", "row"), None), P(("row", "col"), None)), check_vma=False)
```
